32 devices in a mesh: prow: 8 (over z, y), pcol: 4 (over x, core).
Axes of the slice: x: 2, y: 2, z: 4, core: 2. Of those that a mesh axis runs over, the one named last changes fastest.
Arguments:
- iface_tiles: int32 [32, 16], replicated, may hold values from 0 to 63, as said below
- interior_sizes: int32 [32], P(('prow', 'pcol')), may hold values from 128 to 512
- coupling: float32 [32, 512, 2048], P(('prow', 'pcol')), may hold values from -0.25 to 0.25
- factor_inverse: float32 [32, 512, 512], P(('prow', 'pcol')), as said below
- interface_block: float32 [8, 8, 4, 16, 128, 128], P('prow', None, 'pcol'), as said below
Outputs:
- schur: float32 [8, 8, 4, 16, 128, 128], P('prow', None, 'pcol')
- panel: float32 [8, 8, 128, 128], P('prow', None, 'pcol')
The draws below stay inside these ranges and needn't reach their ends.
Inputs may be any that keep to these rules, and one draw needn't show every extreme that they name: `iface_tiles`: each row holds 16 distinct tile numbers; for every r, exactly 2 of them are r modulo 8; every tile number stands in exactly 8 rows. `factor_inverse`: each matrix is lower triangular with a diagonal between 0.25 and 1. `interface_block`: diagonal entries lie between 80 and 160; other entries are of order one.
All inputs are finite; a program needn't handle non-finite values.
Results may differ from the reference program's by a relative error of at most 0.0001.
Values sent between devices are 32-bit elements; how exact they have to be, the bound alone decides.
No kernel may reach another device: no remote copies, remote signals or barrier semaphores. Data moves between devices by JAX's collectives and lax.ppermute only.
A program may use at most 128 MiB of HBM per device.

```python
import jax
import jax.numpy as jnp
from jax import lax

IFACE = 2048
TILE = 128
NI = 512
LR_DEV = 8
GT = 16
NT = 64
LC = 16
SUBDOMAINS = 32
N_PROW = 8
N_PCOL = 4


def shuffle_row(row_key, values):
    return jax.random.permutation(row_key, values)


def draw_iface_tiles(key, part):
    rows_per = IFACE // TILE // N_PROW
    key_list = jax.random.split(jax.random.fold_in(key, 11), N_PROW)
    orders = jax.vmap(shuffle_row)(key_list, jnp.broadcast_to(jnp.arange(SUBDOMAINS, dtype=jnp.int32), (N_PROW, SUBDOMAINS)))
    quotient = (rows_per * orders.T[:, :, None] + jnp.arange(rows_per, dtype=jnp.int32)[None, None, :]) % LR_DEV
    tile_ids = quotient * N_PROW + jnp.arange(N_PROW, dtype=jnp.int32)[None, :, None]
    tile_ids = tile_ids.reshape(SUBDOMAINS, rows_per * N_PROW).astype(jnp.int32)
    shuffle_keys = jax.random.split(jax.random.fold_in(key, 12), SUBDOMAINS)
    return jax.vmap(shuffle_row)(shuffle_keys, tile_ids).astype(jnp.int32)


def draw_factor_inverse(key, part):
    first_key = jax.random.fold_in(key, 21)
    second_key = jax.random.fold_in(key, 22)
    shape = (SUBDOMAINS, NI, NI)
    noise = jax.random.normal(first_key, shape, jnp.float32) * (0.5 / NI ** 0.5)
    diagonal = jax.random.uniform(second_key, (SUBDOMAINS, NI), jnp.float32, 0.5, 1.0)
    lower = jnp.tril(noise, -1)
    eye_mask = jnp.eye(NI, dtype=jnp.float32)[None, :, :]
    return (lower + eye_mask * diagonal[:, :, None]).astype(jnp.float32)


def draw_interface_block(key, part):
    local_cols = LR_DEV * N_PROW // N_PCOL
    shape = (N_PROW, LR_DEV, N_PCOL, local_cols, TILE, TILE)
    first_key = jax.random.fold_in(key, 31)
    second_key = jax.random.fold_in(key, 32)
    noise = jax.random.normal(first_key, shape, jnp.float32) * 0.5
    diagonal = jax.random.uniform(second_key, shape, jnp.float32, 80.0, 160.0)
    prow_ids = jnp.arange(N_PROW, dtype=jnp.int32)[:, None, None, None, None, None]
    row_tiles = jnp.arange(LR_DEV, dtype=jnp.int32)[None, :, None, None, None, None]
    pcol_ids = jnp.arange(N_PCOL, dtype=jnp.int32)[None, None, :, None, None, None]
    col_tiles = jnp.arange(local_cols, dtype=jnp.int32)[None, None, None, :, None, None]
    inner_rows = jnp.arange(TILE, dtype=jnp.int32)[None, None, None, None, :, None]
    inner_cols = jnp.arange(TILE, dtype=jnp.int32)[None, None, None, None, None, :]
    global_row = (row_tiles * N_PROW + prow_ids) * TILE + inner_rows
    global_col = (col_tiles * N_PCOL + pcol_ids) * TILE + inner_cols
    return jnp.where(global_row == global_col, diagonal, noise).astype(jnp.float32)


def set_ends(entries, stream_key, low, top_value):
    shape = entries.shape
    place = [jax.random.randint(jax.random.fold_in(stream_key, axis), (), 0, shape[axis]) for axis in range(len(shape))]
    entries = entries.at[tuple(place)].set(low)
    longest = shape.index(max(shape))
    place[longest] = (place[longest] + 1) % shape[longest]
    return entries.at[tuple(place)].set(top_value)


def block_scale(stream_key, extent, pieces, smallest, top_value):
    def one(position, shards_of):
        heights = jax.random.uniform(jax.random.fold_in(jax.random.fold_in(stream_key, 6), position), (shards_of,), jnp.float32, smallest / len(pieces), top_value / len(pieces))
        return jnp.repeat(jnp.exp(heights), extent[position] // shards_of).reshape((-1,) + (1,) * (len(extent) - position - 1))

    loudness = one(*pieces[0])
    for cut in pieces[1:]:
        loudness = loudness * one(*cut)
    return loudness


def centred(key, extent, deviation, limit, shards=(), kind=jnp.bfloat16):
    gain = block_scale(key, extent, shards, -0.22, 0.18) if shards else 1.0
    array = jax.random.normal(key, extent, jnp.float32) * deviation * gain
    return jnp.minimum(jnp.maximum(array, -limit), limit).astype(kind)


def setup_inputs(seed: int = 0) -> dict:
    key_of = jax.random.split(jax.random.key(seed), 6)
    iface_tiles = draw_iface_tiles(jax.random.fold_in(key_of[5], 71), 0)
    interior_sizes = set_ends(jax.random.randint(key_of[1], (SUBDOMAINS,), NI // 4, NI + 1), jax.random.fold_in(key_of[1], 1), NI // 4, NI).astype(jnp.int32)
    coupling = centred(key_of[2], (SUBDOMAINS, NI, IFACE), NI ** -0.5, 0.25, ((0, 32),), jnp.float32)
    factor_inverse = draw_factor_inverse(jax.random.fold_in(key_of[5], 71), 0)
    interface_block = draw_interface_block(jax.random.fold_in(key_of[5], 71), 0)
    return {"iface_tiles": iface_tiles, "interior_sizes": interior_sizes, "coupling": coupling, "factor_inverse": factor_inverse, "interface_block": interface_block}


def reference(iface_tiles, interior_sizes, coupling, factor_inverse, interface_block):
    grid_tiles = interface_block.transpose(1, 0, 3, 2, 4, 5).reshape(NT, NT, TILE, TILE)

    def add_domain(index, running):
        live_count = interior_sizes[index]
        row_live = (jnp.arange(NI, dtype=jnp.int32) < live_count)[:, None]
        masked = jnp.where(row_live, coupling[index], 0.0)
        weighted = jnp.dot(factor_inverse[index].astype(jnp.float32), masked.astype(jnp.float32), precision=lax.Precision.HIGHEST, preferred_element_type=jnp.float32)
        weighted = jnp.where(row_live, weighted, 0.0)
        gram = jnp.dot(weighted.T.astype(jnp.float32), weighted.astype(jnp.float32), precision=lax.Precision.HIGHEST, preferred_element_type=jnp.float32)
        tiled = gram.reshape(GT, TILE, GT, TILE).transpose(0, 2, 1, 3)
        tile_ids = iface_tiles[index].astype(jnp.int32)
        return running.at[tile_ids[:, None], tile_ids[None, :]].add(-tiled)
    grid_tiles = lax.fori_loop(0, SUBDOMAINS, add_domain, grid_tiles)
    schur = grid_tiles.reshape(LR_DEV, N_PROW, LC, N_PCOL, TILE, TILE).transpose(1, 0, 3, 2, 4, 5)
    column = grid_tiles[:, 0]
    diag_block = column[0]
    lower = jnp.linalg.cholesky(0.5 * (diag_block + diag_block.T))
    flat = column.reshape(NT * TILE, TILE)
    solved = jax.scipy.linalg.solve_triangular(lower, flat.T, lower=True)
    panel = solved.T.reshape(LR_DEV, N_PROW, TILE, TILE).transpose(1, 0, 2, 3)
    return (schur, panel)
```

```python
import functools

import jax
import jax.numpy as jnp
from jax import lax
from jax.experimental import pallas as pl
from jax.experimental.pallas import tpu as pltpu
from jax.sharding import PartitionSpec as P


def halves(x):
    high = x.astype(jnp.bfloat16)
    low = (x - high.astype(jnp.float32)).astype(jnp.bfloat16)
    return high, low


def left_stack(x):
    high, low = halves(x)
    return jnp.concatenate([high, high, low], axis=1)


def right_stack(x):
    high, low = halves(x)
    return jnp.concatenate([high, low, high], axis=0)


def weigh_body(order_ref, live_ref, factor_ref, first_ref, second_ref, out_ref, factor_scratch):
    @pl.when(pl.program_id(0) == 0)
    def _():
        factor_scratch[...] = left_stack(factor_ref[...])

    block = jnp.concatenate([first_ref[...], second_ref[...]], axis=1)
    live = lax.broadcasted_iota(jnp.int32, block.shape, 0) < live_ref[0]
    block = jnp.where(live, block, 0.0)
    product = jnp.dot(factor_scratch[...], right_stack(block), preferred_element_type=jnp.float32)
    out_ref[...] = jnp.where(live, product, 0.0)


def weigh(order, live_count, factor, coupling, width):
    interior, iface = coupling.shape
    grid_spec = pltpu.PrefetchScalarGridSpec(
        num_scalar_prefetch=2,
        grid=(iface // (2 * width),),
        in_specs=[
            pl.BlockSpec((interior, interior), lambda i, order, live: (0, 0)),
            pl.BlockSpec((interior, width), lambda i, order, live: (0, order[2 * i])),
            pl.BlockSpec((interior, width), lambda i, order, live: (0, order[2 * i + 1])),
        ],
        out_specs=pl.BlockSpec((interior, 2 * width), lambda i, order, live: (0, i)),
        scratch_shapes=[pltpu.VMEM((interior, 3 * interior), jnp.bfloat16)],
    )
    return pl.pallas_call(
        weigh_body,
        grid_spec=grid_spec,
        out_shape=jax.ShapeDtypeStruct((interior, iface), jnp.float32),
        compiler_params=pltpu.CompilerParams(dimension_semantics=("arbitrary",)),
        name="weigh",
    )(order, live_count, factor, coupling, coupling)


def gram_body(left_ref, right_ref, out_ref, right_scratch, *, columns, width, rows_per):
    @pl.when(pl.program_id(0) == 0)
    def _():
        right_scratch[...] = right_stack(right_ref[...])

    left = left_stack(left_ref[...].T)
    for q, positions in enumerate(columns):
        for c, position in enumerate(positions):
            if position % 2:
                continue
            pair = jnp.dot(
                left,
                right_scratch[:, position * width : (position + 2) * width],
                preferred_element_type=jnp.float32,
            )
            for half in range(2):
                qq, cc = owner_of(columns, position + half)
                for r in range(rows_per):
                    out_ref[0, qq, r, cc] = pair[
                        r * width : (r + 1) * width, half * width : (half + 1) * width
                    ]


def owner_of(columns, position):
    for q, positions in enumerate(columns):
        if position in positions:
            return q, positions.index(position)


def gram(weighted, columns, rows_grid, rows_per, width):
    interior, iface = weighted.shape
    block = (len(columns), rows_per, len(columns[0]), width, width)
    return pl.pallas_call(
        functools.partial(gram_body, columns=columns, width=width, rows_per=rows_per),
        grid=(rows_grid,),
        in_specs=[
            pl.BlockSpec((interior, rows_per * width), lambda i: (0, i)),
            pl.BlockSpec((interior, iface), lambda i: (0, 0)),
        ],
        out_specs=pl.BlockSpec((1,) + block, lambda i: (i, 0, 0, 0, 0, 0)),
        out_shape=jax.ShapeDtypeStruct((rows_grid,) + block, jnp.float32),
        scratch_shapes=[pltpu.VMEM((3 * interior, iface), jnp.bfloat16)],
        compiler_params=pltpu.CompilerParams(dimension_semantics=("arbitrary",)),
        name="gram",
    )(weighted, weighted)


def assemble_body(entry_ref, first_ref, target_ref, base_ref, *refs, depth, cols_per):
    out_ref = refs[depth]
    row = pl.program_id(0)
    out_ref[...] = base_ref[...]
    for k in range(depth):
        first = first_ref[row * depth + k]
        for c in range(cols_per):
            target = target_ref[first + c]
            out_ref[0, target] = out_ref[0, target] - refs[k][0, c]


def assemble(entries, firsts, targets, base, received, depth):
    local_rows, local_cols, width, _ = base.shape
    cols_per = received.shape[1]

    def pick(k):
        return lambda i, entry, first, target: (entry[i * depth + k], 0, 0, 0)

    whole = pl.BlockSpec(
        (1, local_cols, width, width), lambda i, entry, first, target: (i, 0, 0, 0)
    )
    grid_spec = pltpu.PrefetchScalarGridSpec(
        num_scalar_prefetch=3,
        grid=(local_rows,),
        in_specs=[whole]
        + [pl.BlockSpec((1, cols_per, width, width), pick(k)) for k in range(depth)],
        out_specs=whole,
    )
    return pl.pallas_call(
        functools.partial(assemble_body, depth=depth, cols_per=cols_per),
        grid_spec=grid_spec,
        out_shape=jax.ShapeDtypeStruct(base.shape, jnp.float32),
        compiler_params=pltpu.CompilerParams(dimension_semantics=("arbitrary",)),
        name="assemble",
    )(entries, firsts, targets, base, *([received] * depth))


def ranks(keys):
    size = keys.shape[-1]
    full = keys * size + lax.iota(jnp.int32, size)
    return jnp.sum((full[..., None, :] < full[..., :, None]).astype(jnp.int32), axis=-1)


def place(rank, values):
    size = rank.shape[-1]
    hit = rank[..., None, :] == lax.iota(jnp.int32, size)[:, None]
    return jnp.sum(jnp.where(hit, values[..., None, :], 0), axis=-1)


def shards(iface_tiles, interior_sizes, coupling, factor_inverse, interface_block):
    rows_grid = lax.axis_size("prow")
    cols_grid = lax.axis_size("pcol")
    prow_index = lax.axis_index("prow")
    pcol_index = lax.axis_index("pcol")
    self_index = prow_index * cols_grid + pcol_index
    domains, tile_count = iface_tiles.shape
    width = interface_block.shape[-1]
    local_rows = interface_block.shape[1]
    local_cols = interface_block.shape[3]
    rows_per = tile_count // rows_grid
    cols_per = tile_count // cols_grid
    depth = domains * rows_per // local_rows
    columns = [
        [r * rows_per + j for r in range(q, rows_grid, cols_grid) for j in range(rows_per)]
        for q in range(cols_grid)
    ]
    rank = ranks(iface_tiles % rows_grid)
    ordered = place(rank, iface_tiles)
    origin = place(rank, jnp.broadcast_to(lax.iota(jnp.int32, tile_count), rank.shape))
    own_order = lax.dynamic_index_in_dim(origin, self_index, 0, keepdims=False)
    own_tiles = lax.dynamic_index_in_dim(ordered, self_index, 0, keepdims=False)

    weighted = weigh(own_order, interior_sizes, factor_inverse[0], coupling[0], width)

    base = interface_block.reshape(local_rows, local_cols, width, width)
    by_row = ordered.reshape(domains, rows_grid, rows_per)
    target_rows = lax.dynamic_index_in_dim(by_row, prow_index, 1, keepdims=False) // rows_grid
    by_col = ordered.reshape(domains, rows_grid // cols_grid, cols_grid, rows_per)
    target_cols = lax.dynamic_index_in_dim(by_col, pcol_index, 2, keepdims=False) // cols_grid

    zero_hits = own_tiles[:rows_per] == 0
    lead = weighted[:, : rows_per * width].reshape(-1, rows_per, width)
    lead = jnp.sum(jnp.where(zero_hits[None, :, None], lead, 0.0), axis=1)
    early = lax.dot_general(
        weighted, lead, (((0,), (0,)), ((), ())), precision=lax.Precision.HIGHEST
    ).reshape(rows_grid, rows_per, width, width)
    early_diag = jnp.sum(
        jnp.where(zero_hits[:, None, None], early[0], 0.0), axis=0
    )
    diag_base = jnp.where(self_index == 0, base[0, 0], 0.0)
    diag_block = lax.psum(diag_base - early_diag, ("prow", "pcol"))
    early = lax.all_to_all(early, "prow", split_axis=0, concat_axis=0, tiled=True)
    early = early.reshape(rows_grid * rows_per, width, width)
    early_rows = target_rows.reshape(rows_grid, cols_grid, rows_per)
    early_rows = lax.dynamic_index_in_dim(early_rows, pcol_index, 1, keepdims=False).reshape(-1)
    hit = early_rows[None, :] == lax.iota(jnp.int32, local_rows)[:, None]
    column = jnp.where(pcol_index == 0, base[:, 0], 0.0) - jnp.sum(
        jnp.where(hit[:, :, None, None], early[None], 0.0), axis=1
    )
    column = lax.psum_scatter(column, "pcol", scatter_dimension=1, tiled=True)
    lower = jnp.linalg.cholesky(0.5 * (diag_block + diag_block.T))
    flat = column.reshape(-1, width)
    panel = jax.scipy.linalg.solve_triangular(lower, flat.T, lower=True).T.reshape(column.shape)

    contribution = gram(weighted, columns, rows_grid, rows_per, width)
    received = lax.all_to_all(
        contribution.reshape(domains, rows_per, cols_per, width, width),
        ("prow", "pcol"),
        split_axis=0,
        concat_axis=0,
        tiled=True,
    )
    flat_rows = target_rows.reshape(-1)
    entries = place(ranks(flat_rows), lax.iota(jnp.int32, flat_rows.shape[0]))
    firsts = entries // rows_per * cols_per
    schur = assemble(
        entries,
        firsts,
        target_cols.reshape(-1),
        base,
        received.reshape(domains * rows_per, cols_per, width, width),
        depth,
    )
    return (schur.reshape(interface_block.shape), panel[None])


def solution(mesh):
    in_specs = (
        P(),
        P(("prow", "pcol")),
        P(("prow", "pcol"), None, None),
        P(("prow", "pcol"), None, None),
        P("prow", None, "pcol", None, None, None),
    )
    out_specs = (P("prow", None, "pcol", None, None, None), P("prow", None, "pcol", None))
    return jax.shard_map(shards, mesh=mesh, in_specs=in_specs, out_specs=out_specs, check_vma=False)
```
